256 devices in a mesh: groups: 4 (over x, y), seq: 32 (over z), head: 2 (over core).
Axes of the slice: x: 2, y: 2, z: 32, core: 2. Of those that a mesh axis runs over, the one named last changes fastest.
The devices are a block of a 4x8x32 slice.
Arguments:
- query_rows: bfloat16 [16384, 4096], P(('groups', 'seq'), 'head'), parts along dimension 0, may hold values from -160 to 160
- key_rows: bfloat16 [16384, 512], P(('groups', 'seq'), 'head'), parts along dimension 0, may hold values from -6 to 6
- value_rows: bfloat16 [16384, 512], P(('groups', 'seq'), 'head'), parts along dimension 0, may hold values from -6 to 6
- grad_out: bfloat16 [16384, 4096], P(('groups', 'seq'), 'head'), parts along dimension 0, may hold values from -6 to 6
- lengths: int32 [512], P(('groups', 'seq')), parts along dimension 0, may hold values from 1 to 2176, as said below
Outputs:
- attended: bfloat16 [16384, 4096], P(('groups', 'seq'), 'head'), parts along dimension 0
- grad_query: bfloat16 [16384, 4096], P(('groups', 'seq'), 'head'), parts along dimension 0
- grad_key: bfloat16 [16384, 512], P(('groups', 'seq'), 'head'), parts along dimension 0
- grad_value: bfloat16 [16384, 512], P(('groups', 'seq'), 'head'), parts along dimension 0
The draws below stay inside these ranges and needn't reach their ends.
There are 4 independent parts, one for each index of `groups`. The reference program is written for one: setup_inputs(seed, part) draws one part's arguments, and reference() takes and returns one part's arrays. A program takes and returns all parts, laid end to end along the dimension named above; each array names one. Nothing has to cross between parts.
Inputs may be any that keep to these rules, and one draw needn't show every extreme that they name: The 128 lengths sum to 4096; the first document is the longest, with exactly 2176 tokens.
All inputs are finite; a program needn't handle non-finite values.
Results may differ from the reference program's by a relative error of at most 0.035.
Values may be sent and summed in bfloat16 or wider, within the bound.
No kernel may reach another device: no remote copies, remote signals or barrier semaphores. Data moves between devices by JAX's collectives and lax.ppermute only.
A program may use at most 64 MiB of HBM per device.

```python
import math
import jax
import jax.numpy as jnp
from jax import lax

HD = 128
QH = 32
KVH = 4
TOKENS = 4096
MOST = 2176
NDOC = 128


def shaped_keys(key):
    base = jnp.clip(jax.random.normal(jax.random.fold_in(key, 5), (TOKENS, KVH, HD), jnp.float32), -6.0, 6.0)
    return base


def draw_key_rows(key, part):
    return shaped_keys(key).reshape(TOKENS, KVH * HD).astype(jnp.bfloat16)


def draw_query_rows(key, part):
    group = QH // KVH
    noise = jnp.clip(jax.random.normal(jax.random.fold_in(key, 3), (TOKENS, KVH, group, HD), jnp.float32), -6.0, 6.0)
    rows = noise
    return rows.reshape(TOKENS, QH * HD).astype(jnp.bfloat16)


def draw_lengths(key, part):
    remain = TOKENS - MOST
    others = NDOC - 1
    order = jax.random.permutation(jax.random.fold_in(key, 11), remain - 1)
    cuts = jnp.sort(order[:others - 1].astype(jnp.int32) + 1)
    edges = jnp.concatenate([jnp.zeros((1,), jnp.int32), cuts, jnp.full((1,), remain, jnp.int32)])
    rest = (edges[1:] - edges[:-1]).astype(jnp.int32)
    return jnp.concatenate([jnp.full((1,), MOST, jnp.int32), rest]).astype(jnp.int32)


def block_levels(own_key, shape, cuts, smallest, top_value):
    gain, own = 1.0, jax.random.fold_in(own_key, 6)
    for dim, parts in cuts:
        heights = jnp.exp(jax.random.uniform(jax.random.fold_in(own, dim), (parts,), jnp.float32, smallest / len(cuts), top_value / len(cuts)))
        gain = gain * jnp.repeat(heights, shape[dim] // parts).reshape([-1 if axis == dim else 1 for axis in range(len(shape))])
    return gain


def gaussian(key, shape, deviation, reach, cuts=(), kind=jnp.bfloat16):
    level = block_levels(key, shape, cuts, -0.22, 0.18) if cuts else 1.0
    values = jax.random.normal(key, shape, jnp.float32) * deviation * level
    return jnp.minimum(jnp.maximum(values, -reach), reach).astype(kind)


def setup_inputs(seed: int = 0, part: int = 0) -> dict:
    keys = jax.random.split(jax.random.key(seed), 6)
    part_keys = jax.random.split(jax.random.fold_in(keys[5], part), 6)
    return {
        "query_rows": draw_query_rows(jax.random.fold_in(jax.random.fold_in(keys[5], part), 71), part),
        "key_rows": draw_key_rows(jax.random.fold_in(jax.random.fold_in(keys[5], part), 71), part),
        "value_rows": gaussian(part_keys[2], (TOKENS, KVH * HD), 1.0, 6.0, ((0, 32), (1, 2))),
        "grad_out": gaussian(part_keys[3], (TOKENS, QH * HD), 1.0, 6.0, ((0, 32), (1, 2))),
        "lengths": draw_lengths(jax.random.fold_in(jax.random.fold_in(keys[5], part), 71), part),
    }


def doc_index(ends, positions):
    return lax.optimization_barrier(jnp.sum((ends[None, :] <= positions[:, None]).astype(jnp.int32), axis=1))

def reference(query_rows, key_rows, value_rows, grad_out, lengths):
    group = QH // KVH
    scale = 1.0 / math.sqrt(HD)
    block = math.gcd(TOKENS, 512)
    window = min(TOKENS, MOST + block)
    count = TOKENS // block
    ends = jnp.cumsum(lengths).astype(jnp.int32)
    queries = query_rows.reshape(TOKENS, KVH, group, HD).astype(jnp.float32)
    keyset = key_rows.reshape(TOKENS, KVH, HD).astype(jnp.float32)
    valueset = value_rows.reshape(TOKENS, KVH, HD).astype(jnp.float32)
    cotangent = grad_out.reshape(TOKENS, KVH, group, HD).astype(jnp.float32)

    def one_block(carry, number):
        key_grad, value_grad = carry
        first = number * block
        key_first = jnp.maximum(first + block - window, 0).astype(jnp.int32)
        query_pos = first + jnp.arange(block, dtype=jnp.int32)
        key_pos = key_first + jnp.arange(window, dtype=jnp.int32)
        allowed = (doc_index(ends, query_pos)[:, None] == doc_index(ends, key_pos)[None, :]) & (key_pos[None, :] <= query_pos[:, None])
        allowed = allowed[:, None, None, :]
        query_block = lax.dynamic_slice_in_dim(queries, first, block, 0)
        grad_block = lax.dynamic_slice_in_dim(cotangent, first, block, 0)
        key_block = lax.dynamic_slice_in_dim(keyset, key_first, window, 0)
        value_block = lax.dynamic_slice_in_dim(valueset, key_first, window, 0)
        scores = scale * jnp.einsum('tagd,kad->tagk', query_block, key_block)
        masked = jnp.where(allowed, scores, -1e+30)
        rowmax = lax.optimization_barrier(jnp.max(masked, axis=-1, keepdims=True))
        expo = jnp.where(allowed, jnp.exp(masked - rowmax), 0.0)
        rowsum = lax.optimization_barrier(jnp.sum(expo, axis=-1, keepdims=True))
        weights = lax.optimization_barrier(expo.astype(jnp.bfloat16)).astype(jnp.float32)
        attended = (jnp.einsum('tagk,kad->tagd', weights, value_block) / rowsum).astype(jnp.bfloat16)
        attended_wide = lax.optimization_barrier(attended).astype(jnp.float32)
        lse = rowmax + jnp.log(rowsum)
        delta = lax.optimization_barrier(jnp.sum(grad_block * attended_wide, axis=-1, keepdims=True))
        prob = jnp.where(allowed, jnp.exp(masked - lse), 0.0)
        prob_low = lax.optimization_barrier(prob.astype(jnp.bfloat16)).astype(jnp.float32)
        value_part = jnp.einsum('tagk,tagd->kad', prob_low, grad_block)
        dprob = jnp.einsum('tagd,kad->tagk', grad_block, value_block)
        dscore = lax.optimization_barrier((prob * (dprob - delta)).astype(jnp.bfloat16)).astype(jnp.float32)
        query_grad = (scale * jnp.einsum('tagk,kad->tagd', dscore, key_block)).astype(jnp.bfloat16)
        key_part = jnp.einsum('tagk,tagd->kad', dscore, query_block)
        old_key = lax.dynamic_slice_in_dim(key_grad, key_first, window, 0)
        old_value = lax.dynamic_slice_in_dim(value_grad, key_first, window, 0)
        key_grad = lax.dynamic_update_slice_in_dim(key_grad, old_key + key_part, key_first, 0)
        value_grad = lax.dynamic_update_slice_in_dim(value_grad, old_value + value_part, key_first, 0)
        return ((key_grad, value_grad), (attended, query_grad))
    start = (jnp.zeros((TOKENS, KVH, HD), jnp.float32), jnp.zeros((TOKENS, KVH, HD), jnp.float32))
    (key_grad, value_grad), (attended, query_grad) = lax.scan(one_block, start, jnp.arange(count, dtype=jnp.int32))
    attended = attended.reshape(TOKENS, QH * HD)
    query_grad = query_grad.reshape(TOKENS, QH * HD)
    key_out = (scale * key_grad).astype(jnp.bfloat16).reshape(TOKENS, KVH * HD)
    value_out = value_grad.astype(jnp.bfloat16).reshape(TOKENS, KVH * HD)
    return (attended, query_grad, key_out, value_out)
```

```python
import functools
import math

import jax
import jax.numpy as jnp
from jax import lax
from jax.experimental import pallas as pl
from jax.experimental.pallas import tpu as pltpu
from jax.sharding import PartitionSpec as P

HD = 128
MOST = 2176
NEGATIVE = -1e30
SCALE = 1.0 / math.sqrt(HD)
LOG2E = math.log2(math.e)
C2 = SCALE * LOG2E

F32 = jnp.float32
BF16 = jnp.bfloat16

FORWARD_CALLS = ((0, 1, 2, 3, 4), (5, 6, 7, 8), (9, 10, 11, 12), (13, 14, 15), (16,))
BACKWARD_CALLS = ((16,), (15, 14), (13, 12, 11), (10, 9, 8), (7, 6, 5), (4, 3, 2), (1, 0))


def mm(a, b):
    return jnp.dot(a, b, preferred_element_type=F32)


def mm_tn(a, b):
    return lax.dot_general(a, b, (((0,), (0,)), ((), ())), preferred_element_type=F32)


def allowed_of(start, off, index, tok, shape):
    key = lax.broadcasted_iota(jnp.int32, shape, 0)
    keep = key >= start - (index - off) * tok
    if off == 0:
        query = lax.broadcasted_iota(jnp.int32, shape, 1) % tok
        keep = keep & (key <= query)
    return keep


def forward_kernel(offs, first, last, tok, group, *refs):
    count = len(offs)
    info, qt, start = refs[:3]
    kvs = refs[3 : 3 + count]
    rest = refs[3 + count :]
    if not first:
        m_in, l_in, acc_in = rest[:3]
        rest = rest[3:]
    if last:
        dot, att_out, lse_out, delta_out = rest[:4]
        m, l, acc = rest[4:]
    else:
        m, l, acc = rest
    index, reach = info[0], info[1]
    if first:
        m[0] = jnp.full(m.shape[1:], NEGATIVE, F32)
        l[0] = jnp.zeros(l.shape[1:], F32)
        acc[0] = jnp.zeros(acc.shape[1:], F32)
    else:
        m[0] = m_in[0]
        l[0] = l_in[0]
        acc[0] = acc_in[0]

    for off, kv in zip(offs, kvs):

        @pl.when(off <= reach)
        def _(off=off, kv=kv):
            scores = mm(kv[0, 0], qt[0])
            keep = allowed_of(start[...], off, index, tok, scores.shape)
            scores = jnp.where(keep, scores, NEGATIVE)
            old = m[0]
            new = jnp.maximum(old, jnp.max(scores, axis=0, keepdims=True))
            factor = jnp.exp2((old - new) * C2)
            expo = jnp.exp2((scores - new) * C2)
            m[0] = new
            l[0] = l[0] * factor + jnp.sum(expo, axis=0, keepdims=True)
            acc[0] = acc[0] * factor + mm_tn(kv[1, 0], expo.astype(BF16))

    if last:
        att = (acc[0] / l[0]).astype(BF16)
        lse_out[0] = m[0] * C2 + jnp.log2(l[0])
        wide = att.astype(F32)
        delta_out[0] = jnp.sum(wide * dot[0].astype(F32), axis=0, keepdims=True)
        for h in range(group):
            att_out[:, h * HD : (h + 1) * HD] = wide[:, h * tok : (h + 1) * tok].T.astype(BF16)


def backward_kernel(offs, first, last, tok, group, *refs):
    count = len(offs)
    info, qt, qn, dot, don, lse, delta, start = refs[:8]
    kvs = refs[8 : 8 + count]
    rest = refs[8 + count :]
    if not first:
        dq_in = rest[0]
        rest = rest[1:]
    outs = rest[:count]
    rest = rest[count:]
    if last:
        dq_out, dq = rest
    else:
        (dq,) = rest
    index, reach = info[0], info[1]
    if first:
        dq[0] = jnp.zeros(dq.shape[1:], F32)
    else:
        dq[0] = dq_in[0]

    for off, kv, out in zip(offs, kvs, outs):

        @pl.when(off <= reach)
        def _(off=off, kv=kv, out=out):
            scores = mm(kv[0, 0], qt[0])
            keep = allowed_of(start[...], off, index, tok, scores.shape)
            prob = jnp.exp2(jnp.where(keep, scores * C2 - lse[0], NEGATIVE))
            out[1, 0] = mm(prob.astype(BF16), don[0])
            dscore = (prob * (mm(kv[1, 0], dot[0]) - delta[0])).astype(BF16)
            out[0, 0] = mm(dscore, qn[0])
            dq[0] += mm_tn(kv[0, 0], dscore)

        @pl.when(off > reach)
        def _(out=out):
            out[...] = jnp.zeros(out.shape, F32)

    if last:
        total = dq[0] * SCALE
        for h in range(group):
            dq_out[:, h * HD : (h + 1) * HD] = total[:, h * tok : (h + 1) * tok].T.astype(BF16)


def by_head(*shape):
    zeros = (0,) * (len(shape) - 1)
    return pl.BlockSpec((1, *shape[1:]), lambda g, info: (g, *zeros))


def forward(offs, first, last, tok, info, qt, start, kvs, state, dot):
    kv_heads, _, wide = qt.shape
    group = wide // tok
    row = by_head(kv_heads, 1, wide)
    square = by_head(kv_heads, HD, wide)
    kv_spec = pl.BlockSpec((2, 1, tok, HD), lambda g, info: (0, g, 0, 0))
    in_specs = [square, pl.BlockSpec((1, wide), lambda g, info: (0, 0))] + [kv_spec] * len(kvs)
    args = [qt, start, *kvs]
    row_shape = jax.ShapeDtypeStruct((kv_heads, 1, wide), F32)
    square_shape = jax.ShapeDtypeStruct((kv_heads, HD, wide), F32)
    if not first:
        in_specs += [row, row, square]
        args += list(state)
    scratch = []
    if last:
        in_specs.append(square)
        args.append(dot)
        out_specs = [pl.BlockSpec((tok, group * HD), lambda g, info: (0, g)), row, row]
        out_shape = [jax.ShapeDtypeStruct((tok, kv_heads * group * HD), BF16), row_shape, row_shape]
        scratch = [pltpu.VMEM((1, 1, wide), F32), pltpu.VMEM((1, 1, wide), F32), pltpu.VMEM((1, HD, wide), F32)]
    else:
        out_specs = [row, row, square]
        out_shape = [row_shape, row_shape, square_shape]
    return pl.pallas_call(
        functools.partial(forward_kernel, offs, first, last, tok, group),
        out_shape=out_shape,
        grid_spec=pltpu.PrefetchScalarGridSpec(
            num_scalar_prefetch=1,
            grid=(kv_heads,),
            in_specs=in_specs,
            out_specs=out_specs,
            scratch_shapes=scratch,
        ),
        compiler_params=pltpu.CompilerParams(dimension_semantics=("arbitrary",)),
        cost_estimate=pl.CostEstimate(
            flops=4 * len(offs) * kv_heads * tok * wide * HD,
            transcendentals=len(offs) * kv_heads * tok * wide,
            bytes_accessed=8 * kv_heads * HD * wide,
        ),
        name="forward",
    )(info, *args)


def backward(offs, first, last, tok, info, qt, qn, dot, don, lse, delta, start, kvs, dq):
    kv_heads, _, wide = qt.shape
    group = wide // tok
    row = by_head(kv_heads, 1, wide)
    square = by_head(kv_heads, HD, wide)
    tall = by_head(kv_heads, wide, HD)
    kv_spec = pl.BlockSpec((2, 1, tok, HD), lambda g, info: (0, g, 0, 0))
    in_specs = [square, tall, square, tall, row, row, pl.BlockSpec((1, wide), lambda g, info: (0, 0))]
    in_specs += [kv_spec] * len(kvs)
    args = [qt, qn, dot, don, lse, delta, start, *kvs]
    if not first:
        in_specs.append(square)
        args.append(dq)
    out_specs = [kv_spec] * len(kvs)
    out_shape = [jax.ShapeDtypeStruct((2, kv_heads, tok, HD), F32)] * len(kvs)
    scratch = []
    if last:
        out_specs.append(pl.BlockSpec((tok, group * HD), lambda g, info: (0, g)))
        out_shape.append(jax.ShapeDtypeStruct((tok, kv_heads * group * HD), BF16))
        scratch = [pltpu.VMEM((1, HD, wide), F32)]
    else:
        out_specs.append(square)
        out_shape.append(jax.ShapeDtypeStruct((kv_heads, HD, wide), F32))
    return pl.pallas_call(
        functools.partial(backward_kernel, offs, first, last, tok, group),
        out_shape=out_shape,
        grid_spec=pltpu.PrefetchScalarGridSpec(
            num_scalar_prefetch=1,
            grid=(kv_heads,),
            in_specs=in_specs,
            out_specs=out_specs,
            scratch_shapes=scratch,
        ),
        compiler_params=pltpu.CompilerParams(dimension_semantics=("arbitrary",)),
        cost_estimate=pl.CostEstimate(
            flops=10 * len(offs) * kv_heads * tok * wide * HD,
            transcendentals=len(offs) * kv_heads * tok * wide,
            bytes_accessed=12 * kv_heads * HD * wide,
        ),
        name="backward",
    )(info, *args)


def calls(wanted, reach, down):
    kept = [tuple(o for o in offs if o <= reach) for offs in wanted]
    kept = [offs for offs in kept if offs]
    held = sorted(o for offs in kept for o in offs)
    extra = [(o,) for o in range(reach + 1) if o not in held]
    return extra[::-1] + kept if down else kept + extra


def start_of_documents(lengths, tok, index):
    devices = lax.axis_size("seq")
    have = lengths[None]
    while have.shape[0] < devices:
        held = have.shape[0]
        take = min(held, devices - held)
        route = [(i, (i + held) % devices) for i in range(devices)]
        have = jnp.concatenate([have, lax.ppermute(have[:take], "seq", route)])
    each = lengths.shape[0]
    owner = (index - jnp.arange(devices, dtype=jnp.int32)) % devices
    number = (owner[:, None] * each + jnp.arange(each, dtype=jnp.int32)[None]).reshape(-1)
    flat = have.reshape(-1)
    ends = jnp.sum(jnp.where(number[None] <= number[:, None], flat[None], 0), axis=1)
    position = index * tok + jnp.arange(tok, dtype=jnp.int32)
    return jnp.max(jnp.where(ends[None] <= position[:, None], ends[None], 0), axis=1)


def shards(query_rows, key_rows, value_rows, grad_out, lengths):
    tok = query_rows.shape[0]
    kv_heads = key_rows.shape[1] // HD
    q_heads = query_rows.shape[1] // HD
    group = q_heads // kv_heads
    wide = group * tok
    devices = lax.axis_size("seq")
    index = lax.axis_index("seq")
    assert MOST % tok == 0
    edge = MOST // tok
    reach = max(edge, devices - edge) - 1
    up = [(i, i + 1) for i in range(devices - 1) if i + 1 != edge]
    down = [(i + 1, i) for i in range(devices - 1) if i + 1 != edge]

    def heads_apart(rows):
        return rows.reshape(tok, kv_heads, HD).transpose(1, 0, 2)

    def heads_together(blocks):
        return blocks.transpose(1, 0, 2).reshape(tok, kv_heads * HD)

    block = jnp.stack([heads_apart(key_rows), heads_apart(value_rows)])
    blocks = [block]
    for _ in range(reach):
        blocks.append(lax.ppermute(blocks[-1], "seq", up))

    starts = start_of_documents(lengths, tok, index)
    middle = reach // 2
    starts, blocks[middle] = lax.optimization_barrier((starts, blocks[middle]))
    for k in range(middle + 1, reach + 1):
        blocks[k] = lax.ppermute(blocks[k - 1], "seq", up)
    back = index - starts[0] // tok
    info = jnp.stack([index, back]).astype(jnp.int32)
    start = jnp.tile(starts[None], (1, group))

    four = query_rows.reshape(tok, kv_heads, group, HD)
    grad_four = grad_out.reshape(tok, kv_heads, group, HD)
    qt = four.transpose(1, 3, 2, 0).reshape(kv_heads, HD, wide)
    qn = four.transpose(1, 2, 0, 3).reshape(kv_heads, wide, HD)
    dot = grad_four.transpose(1, 3, 2, 0).reshape(kv_heads, HD, wide)
    don = grad_four.transpose(1, 2, 0, 3).reshape(kv_heads, wide, HD)

    groups = calls(FORWARD_CALLS, reach, False)
    state = None
    for n, offs in enumerate(groups):
        state = forward(
            offs, n == 0, n == len(groups) - 1, tok, info, qt, start, [blocks[o] for o in offs], state, dot
        )
    attended, lse, delta = state

    groups = calls(BACKWARD_CALLS, reach, True)
    dq = None
    moving = None
    for n, offs in enumerate(groups):
        *fresh, dq = backward(
            offs, n == 0, n == len(groups) - 1, tok, info, qt, qn, dot, don, lse, delta, start,
            [blocks[o] for o in offs], dq,
        )
        for off, own in zip(offs, fresh):
            total = own if moving is None else own + moving.astype(F32)
            if off:
                moving = lax.ppermute(total.astype(BF16), "seq", down)
    key_out = heads_together((total[0] * SCALE).astype(BF16))
    value_out = heads_together(total[1].astype(BF16))
    return attended, dq, key_out, value_out


def solution(mesh):
    rows = P(("groups", "seq"), "head")
    return jax.shard_map(
        shards,
        mesh=mesh,
        in_specs=(rows, rows, rows, rows, P(("groups", "seq"))),
        out_specs=(rows, rows, rows, rows),
        check_vma=False,
    )
```

```python
import functools
import math

import jax
import jax.numpy as jnp
from jax import lax
from jax.experimental import pallas as pl
from jax.experimental.pallas import tpu as pltpu
from jax.sharding import PartitionSpec as P

HD = 128
MOST = 2176
NEGATIVE = -1e30
SCALE = 1.0 / math.sqrt(HD)
LOG2E = math.log2(math.e)
C2 = SCALE * LOG2E

F32 = jnp.float32
BF16 = jnp.bfloat16

FORWARD_SIZE = 4
BACKWARD_CALLS = ((16,), (15, 14), (13, 12, 11), (10, 9, 8), (7, 6, 5), (4, 3, 2), (1, 0))


def mm(a, b):
    return jnp.dot(a, b, preferred_element_type=F32)


def mm_tn(a, b):
    return lax.dot_general(a, b, (((0,), (0,)), ((), ())), preferred_element_type=F32)


def allowed_of(start, off, index, tok, shape):
    key = lax.broadcasted_iota(jnp.int32, shape, 0)
    keep = key >= start - (index - off) * tok
    if off == 0:
        query = lax.broadcasted_iota(jnp.int32, shape, 1) % tok
        keep = keep & (key <= query)
    return keep


def visit(key, value, qt, keep, m, l, acc):
    scores = mm(key, qt[0])
    if keep is not None:
        scores = jnp.where(keep, scores, NEGATIVE)
    old = m[0]
    new = jnp.maximum(old, jnp.max(scores, axis=0, keepdims=True))
    factor = jnp.exp2((old - new) * C2)
    expo = jnp.exp2((scores - new) * C2)
    m[0] = new
    l[0] = l[0] * factor + jnp.sum(expo, axis=0, keepdims=True)
    acc[0] = acc[0] * factor + mm_tn(value, expo.astype(BF16))


def clear(m, l, acc):
    m[0] = jnp.full(m.shape[1:], NEGATIVE, F32)
    l[0] = jnp.zeros(l.shape[1:], F32)
    acc[0] = jnp.zeros(acc.shape[1:], F32)


def forward_kernel(offs, first, tok, *refs):
    count = len(offs)
    info, qt = refs[:2]
    pairs = refs[2 : 2 + count]
    rest = refs[2 + count :]
    m, l, acc = rest[-3:]
    if first:
        clear(m, l, acc)
    else:
        for here, there in zip(rest[-3:], rest[:3]):
            here[0] = there[0]

    for off, pair in zip(offs, pairs):

        @pl.when(off <= info[0])
        def _(off=off, pair=pair):
            keep = None
            if off == 0:
                shape = (tok, qt.shape[-1])
                keep = lax.broadcasted_iota(jnp.int32, shape, 0) <= lax.broadcasted_iota(jnp.int32, shape, 1) % tok
            visit(pair[0, 0], pair[1, 0], qt, keep, m, l, acc)


def finish_kernel(offs, tok, group, *refs):
    count = len(offs)
    info, qt, start, stack = refs[:4]
    pairs = refs[4 : 4 + count]
    m_in, l_in, acc_in, dot, att_out, lse_out, delta_out, m, l, acc = refs[4 + count :]
    within, index, back = info[0], info[1], info[2]

    @pl.when(within >= 0)
    def _():
        m[0] = m_in[0]
        l[0] = l_in[0]
        acc[0] = acc_in[0]
        for off, pair in zip(offs, pairs):

            @pl.when(off <= within)
            def _(pair=pair):
                visit(pair[0, 0], pair[1, 0], qt, None, m, l, acc)

    @pl.when(within < 0)
    def _():
        clear(m, l, acc)

        def turn(off, _):
            shape = (tok, qt.shape[-1])
            key = lax.broadcasted_iota(jnp.int32, shape, 0)
            query = lax.broadcasted_iota(jnp.int32, shape, 1) % tok
            keep = (key >= start[...] - (index - off) * tok) & (key <= query + off * tok)
            visit(stack[off, 0, 0], stack[off, 1, 0], qt, keep, m, l, acc)
            return 0

        lax.fori_loop(0, jnp.minimum(back, stack.shape[0] - 1) + 1, turn, 0)

    att = (acc[0] / l[0]).astype(BF16)
    lse_out[0] = m[0] * C2 + jnp.log2(l[0])
    wide = att.astype(F32)
    delta_out[0] = jnp.sum(wide * dot[0].astype(F32), axis=0, keepdims=True)
    for h in range(group):
        att_out[:, h * HD : (h + 1) * HD] = wide[:, h * tok : (h + 1) * tok].T.astype(BF16)


def backward_kernel(offs, first, last, tok, group, *refs):
    count = len(offs)
    info, qt, qn, dot, don, lse, delta, start = refs[:8]
    pairs = refs[8 : 8 + count]
    rest = refs[8 + count :]
    if not first:
        dq_in = rest[0]
        rest = rest[1:]
    outs = rest[:count]
    rest = rest[count:]
    if last:
        dq_out, dq = rest
    else:
        (dq,) = rest
    index, back = info[1], info[2]
    if first:
        dq[0] = jnp.zeros(dq.shape[1:], F32)
    else:
        dq[0] = dq_in[0]

    for off, pair, out in zip(offs, pairs, outs):

        @pl.when(off <= back)
        def _(off=off, pair=pair, out=out):
            key, value = pair[0, 0], pair[1, 0]
            scores = mm(key, qt[0])
            keep = allowed_of(start[...], off, index, tok, scores.shape)
            prob = jnp.exp2(jnp.where(keep, scores * C2 - lse[0], NEGATIVE))
            out[1, 0] = mm(prob.astype(BF16), don[0])
            dscore = (prob * (mm(value, dot[0]) - delta[0])).astype(BF16)
            out[0, 0] = mm(dscore, qn[0])
            dq[0] += mm_tn(key, dscore)

        @pl.when(off > back)
        def _(out=out):
            out[...] = jnp.zeros(out.shape, F32)

    if last:
        total = dq[0] * SCALE
        for h in range(group):
            dq_out[:, h * HD : (h + 1) * HD] = total[:, h * tok : (h + 1) * tok].T.astype(BF16)


def by_head(*shape):
    zeros = (0,) * (len(shape) - 1)
    return pl.BlockSpec((1, *shape[1:]), lambda g, info: (g, *zeros))


def forward(offs, first, tok, info, qt, pairs, state):
    kv_heads, _, wide = qt.shape
    row = by_head(kv_heads, 1, wide)
    square = by_head(kv_heads, HD, wide)
    own = pl.BlockSpec((2, 1, tok, HD), lambda g, info: (0, g, 0, 0))
    row_shape = jax.ShapeDtypeStruct((kv_heads, 1, wide), F32)
    return pl.pallas_call(
        functools.partial(forward_kernel, offs, first, tok),
        out_shape=[row_shape, row_shape, jax.ShapeDtypeStruct((kv_heads, HD, wide), F32)],
        grid_spec=pltpu.PrefetchScalarGridSpec(
            num_scalar_prefetch=1,
            grid=(kv_heads,),
            in_specs=[square] + [own] * len(offs) + ([] if first else [row, row, square]),
            out_specs=[row, row, square],
        ),
        compiler_params=pltpu.CompilerParams(dimension_semantics=("arbitrary",)),
        cost_estimate=pl.CostEstimate(
            flops=4 * len(offs) * kv_heads * tok * wide * HD,
            transcendentals=len(offs) * kv_heads * tok * wide,
            bytes_accessed=8 * kv_heads * HD * wide,
        ),
        name="forward",
    )(info, qt, *pairs, *([] if first else state))


def finish(offs, tok, info, qt, start, stack, pairs, state, dot):
    kv_heads, _, wide = qt.shape
    group = wide // tok
    row = by_head(kv_heads, 1, wide)
    square = by_head(kv_heads, HD, wide)
    own = pl.BlockSpec((2, 1, tok, HD), lambda g, info: (0, g, 0, 0))
    whole = pl.BlockSpec((stack.shape[0], 2, 1, tok, HD), lambda g, info: (0, 0, g, 0, 0))
    row_shape = jax.ShapeDtypeStruct((kv_heads, 1, wide), F32)
    return pl.pallas_call(
        functools.partial(finish_kernel, offs, tok, group),
        out_shape=[jax.ShapeDtypeStruct((tok, kv_heads * group * HD), BF16), row_shape, row_shape],
        grid_spec=pltpu.PrefetchScalarGridSpec(
            num_scalar_prefetch=1,
            grid=(kv_heads,),
            in_specs=[square, pl.BlockSpec((1, wide), lambda g, info: (0, 0)), whole]
            + [own] * len(offs)
            + [row, row, square, square],
            out_specs=[pl.BlockSpec((tok, group * HD), lambda g, info: (0, g)), row, row],
            scratch_shapes=[
                pltpu.VMEM((1, 1, wide), F32),
                pltpu.VMEM((1, 1, wide), F32),
                pltpu.VMEM((1, HD, wide), F32),
            ],
        ),
        compiler_params=pltpu.CompilerParams(dimension_semantics=("arbitrary",)),
        cost_estimate=pl.CostEstimate(
            flops=8 * kv_heads * tok * wide * HD,
            transcendentals=2 * kv_heads * tok * wide,
            bytes_accessed=8 * kv_heads * HD * wide,
        ),
        name="finish",
    )(info, qt, start, stack, *pairs, *state, dot)


def backward(offs, first, last, tok, info, qt, qn, dot, don, lse, delta, start, pairs, dq):
    kv_heads, _, wide = qt.shape
    group = wide // tok
    row = by_head(kv_heads, 1, wide)
    square = by_head(kv_heads, HD, wide)
    tall = by_head(kv_heads, wide, HD)
    own = pl.BlockSpec((2, 1, tok, HD), lambda g, info: (0, g, 0, 0))
    in_specs = [square, tall, square, tall, row, row, pl.BlockSpec((1, wide), lambda g, info: (0, 0))]
    in_specs += [own] * len(offs)
    args = [qt, qn, dot, don, lse, delta, start, *pairs]
    if not first:
        in_specs.append(square)
        args.append(dq)
    out_specs = [own] * len(offs)
    out_shape = [jax.ShapeDtypeStruct((2, kv_heads, tok, HD), F32)] * len(offs)
    scratch = []
    if last:
        out_specs.append(pl.BlockSpec((tok, group * HD), lambda g, info: (0, g)))
        out_shape.append(jax.ShapeDtypeStruct((tok, kv_heads * group * HD), BF16))
        scratch = [pltpu.VMEM((1, HD, wide), F32)]
    else:
        out_specs.append(square)
        out_shape.append(jax.ShapeDtypeStruct((kv_heads, HD, wide), F32))
    return pl.pallas_call(
        functools.partial(backward_kernel, offs, first, last, tok, group),
        out_shape=out_shape,
        grid_spec=pltpu.PrefetchScalarGridSpec(
            num_scalar_prefetch=1,
            grid=(kv_heads,),
            in_specs=in_specs,
            out_specs=out_specs,
            scratch_shapes=scratch,
        ),
        compiler_params=pltpu.CompilerParams(dimension_semantics=("arbitrary",)),
        cost_estimate=pl.CostEstimate(
            flops=10 * len(offs) * kv_heads * tok * wide * HD,
            transcendentals=len(offs) * kv_heads * tok * wide,
            bytes_accessed=12 * kv_heads * HD * wide,
        ),
        name="backward",
    )(info, *args)


def backward_calls(reach):
    kept = [tuple(o for o in offs if o <= reach) for offs in BACKWARD_CALLS]
    kept = [offs for offs in kept if offs]
    return [(o,) for o in range(reach, kept[0][0], -1)] + kept


def length_route(devices):
    turn = lambda i, c: (i + 1 - 2 * c) % devices
    return [(2 * i + c, 2 * turn(i, c) + c) for i in range(devices) for c in range(2)]


def start_of_documents(lengths, heard, tok, devices, index):
    half = len(heard)
    mine = jnp.concatenate(heard)
    theirs = lax.ppermute(mine, "head", [(0, 1), (1, 0)])
    sign = jnp.where(lax.axis_index("head") == 0, -1, 1)
    steps = jnp.arange(1, half + 1, dtype=jnp.int32)
    left = devices - 1 - half
    owners = jnp.concatenate([index[None], index + sign * steps, index - sign * steps[:left]]) % devices
    every = jnp.concatenate([lengths[None], mine, theirs[:left]]).reshape(-1)
    each = lengths.shape[0]
    numbers = (owners[:, None] * each + jnp.arange(each, dtype=jnp.int32)[None]).reshape(-1)
    ends = jnp.sum(jnp.where(numbers[None] <= numbers[:, None], every[None], 0), axis=1)
    position = index * tok + jnp.arange(tok, dtype=jnp.int32)
    return jnp.max(jnp.where(ends[None] <= position[:, None], ends[None], 0), axis=1)


def shards(query_rows, key_rows, value_rows, grad_out, lengths):
    tok = query_rows.shape[0]
    kv_heads = key_rows.shape[1] // HD
    q_heads = query_rows.shape[1] // HD
    group = q_heads // kv_heads
    wide = group * tok
    devices = lax.axis_size("seq")
    index = lax.axis_index("seq")
    assert MOST % tok == 0
    edge = MOST // tok
    beyond = devices - edge
    reach = max(edge, beyond) - 1
    up = [(i, (i + 1) % devices) for i in range(devices)]
    down = [((i + 1) % devices, i) for i in range(devices)]

    def heads_apart(rows):
        return rows.reshape(tok, kv_heads, HD).transpose(1, 0, 2)

    def heads_together(blocks):
        return blocks.transpose(1, 0, 2).reshape(tok, kv_heads * HD)

    pairs = [jnp.stack([heads_apart(key_rows), heads_apart(value_rows)])]
    half = devices // 2
    assert lax.axis_size("head") == 2
    heard = [lengths[None]]
    for step in range(max(reach, half)):
        if step < half:
            heard.append(lax.ppermute(heard[-1], ("seq", "head"), length_route(devices)))
        if step < reach:
            pairs.append(lax.ppermute(pairs[-1], "seq", up))
            heard[-1], pairs[-1] = lax.optimization_barrier((heard[-1], pairs[-1]))

    four = query_rows.reshape(tok, kv_heads, group, HD)
    grad_four = grad_out.reshape(tok, kv_heads, group, HD)
    qt = four.transpose(1, 3, 2, 0).reshape(kv_heads, HD, wide)
    qn = four.transpose(1, 2, 0, 3).reshape(kv_heads, wide, HD)
    dot = grad_four.transpose(1, 3, 2, 0).reshape(kv_heads, HD, wide)
    don = grad_four.transpose(1, 2, 0, 3).reshape(kv_heads, wide, HD)

    within = jnp.where(index < edge, index, -1)
    early = jnp.stack([within, index]).astype(jnp.int32)
    state = None
    for at in range(0, reach, FORWARD_SIZE):
        offs = tuple(range(at, min(at + FORWARD_SIZE, reach)))
        state = forward(offs, at == 0, tok, early, qt, [pairs[o] for o in offs], state)

    starts = start_of_documents(lengths, heard[1:], tok, devices, index)
    back = index - starts[0] // tok
    info = jnp.stack([within, index, back]).astype(jnp.int32)
    start = jnp.tile(starts[None], (1, group))
    attended, lse, delta = finish(
        (reach,), tok, info, qt, start, jnp.stack(pairs[:beyond]), [pairs[reach]], state, dot
    )

    groups = backward_calls(reach)
    fresh = {}
    dq = None
    moving = None

    def run(n, dq):
        offs = groups[n]
        *grads, dq = backward(
            offs, n == 0, n == len(groups) - 1, tok, info, qt, qn, dot, don, lse, delta, start,
            [pairs[o] for o in offs], dq,
        )
        fresh.update(zip(offs, grads))
        return dq

    dq = run(0, dq)
    if len(groups) > 1:
        dq = run(1, dq)
    for n, offs in enumerate(groups):
        for off in offs:
            if moving is not None and off == offs[0] and 0 < n < len(groups) - 1:
                dq, moving = lax.optimization_barrier((dq, moving))
                dq = run(n + 1, dq)
            total = fresh[off]
            if moving is not None:
                total = total + moving.astype(F32)
            if off:
                moving = lax.ppermute(total.astype(BF16), "seq", down)
    key_out = heads_together((total[0] * SCALE).astype(BF16))
    value_out = heads_together(total[1].astype(BF16))
    return attended, dq, key_out, value_out


def solution(mesh):
    rows = P(("groups", "seq"), "head")
    return jax.shard_map(
        shards,
        mesh=mesh,
        in_specs=(rows, rows, rows, rows, P(("groups", "seq"))),
        out_specs=(rows, rows, rows, rows),
        check_vma=False,
    )
```

```python
import functools
import math

import jax
import jax.numpy as jnp
from jax import lax
from jax.experimental import pallas as pl
from jax.experimental.pallas import tpu as pltpu
from jax.sharding import PartitionSpec as P

HD = 128
MOST = 2176
NEGATIVE = -1e30
SCALE = 1.0 / math.sqrt(HD)
LOG2E = math.log2(math.e)
C2 = SCALE * LOG2E

F32 = jnp.float32
BF16 = jnp.bfloat16

FORWARD_SIZE = 4
BACKWARD_CALLS = ((16,), (15, 14), (13, 12, 11), (10, 9, 8), (7, 6, 5), (4, 3, 2), (1, 0))


def mm(a, b):
    return jnp.dot(a, b, preferred_element_type=F32)


def mm_tn(a, b):
    return lax.dot_general(a, b, (((0,), (0,)), ((), ())), preferred_element_type=F32)


def allowed_of(start, off, index, tok, shape):
    key = lax.broadcasted_iota(jnp.int32, shape, 0)
    keep = key >= start - (index - off) * tok
    if off == 0:
        query = lax.broadcasted_iota(jnp.int32, shape, 1) % tok
        keep = keep & (key <= query)
    return keep


def visit(key, value, qt, keep, m, l, acc):
    scores = mm(key, qt[0])
    if keep is not None:
        scores = jnp.where(keep, scores, NEGATIVE)
    old = m[0]
    new = jnp.maximum(old, jnp.max(scores, axis=0, keepdims=True))
    factor = jnp.exp2((old - new) * C2)
    expo = jnp.exp2((scores - new) * C2)
    m[0] = new
    l[0] = l[0] * factor + jnp.sum(expo, axis=0, keepdims=True)
    acc[0] = acc[0] * factor + mm_tn(value, expo.astype(BF16))


def clear(m, l, acc):
    m[0] = jnp.full(m.shape[1:], NEGATIVE, F32)
    l[0] = jnp.zeros(l.shape[1:], F32)
    acc[0] = jnp.zeros(acc.shape[1:], F32)


def forward_kernel(offs, first, tok, *refs):
    count = len(offs)
    info, qt = refs[:2]
    pairs = refs[2 : 2 + count]
    rest = refs[2 + count :]
    m, l, acc = rest[-3:]
    if first:
        clear(m, l, acc)
    else:
        for here, there in zip(rest[-3:], rest[:3]):
            here[0] = there[0]

    for off, pair in zip(offs, pairs):

        @pl.when(off <= info[0])
        def _(off=off, pair=pair):
            keep = None
            if off == 0:
                shape = (tok, qt.shape[-1])
                keep = lax.broadcasted_iota(jnp.int32, shape, 0) <= lax.broadcasted_iota(jnp.int32, shape, 1) % tok
            visit(pair[0, 0], pair[1, 0], qt, keep, m, l, acc)


def finish_kernel(offs, tok, group, *refs):
    count = len(offs)
    info, qt, start, stack = refs[:4]
    pairs = refs[4 : 4 + count]
    m_in, l_in, acc_in, dot, att_out, lse_out, delta_out, m, l, acc = refs[4 + count :]
    within, index, back = info[0], info[1], info[2]

    @pl.when(within >= 0)
    def _():
        m[0] = m_in[0]
        l[0] = l_in[0]
        acc[0] = acc_in[0]
        for off, pair in zip(offs, pairs):

            @pl.when(off <= within)
            def _(pair=pair):
                visit(pair[0, 0], pair[1, 0], qt, None, m, l, acc)

    @pl.when(within < 0)
    def _():
        clear(m, l, acc)

        def turn(off, _):
            shape = (tok, qt.shape[-1])
            key = lax.broadcasted_iota(jnp.int32, shape, 0)
            query = lax.broadcasted_iota(jnp.int32, shape, 1) % tok
            keep = (key >= start[...] - (index - off) * tok) & (key <= query + off * tok)
            visit(stack[off, 0, 0], stack[off, 1, 0], qt, keep, m, l, acc)
            return 0

        lax.fori_loop(0, jnp.minimum(back, stack.shape[0] - 1) + 1, turn, 0)

    att = (acc[0] / l[0]).astype(BF16)
    lse_out[0] = m[0] * C2 + jnp.log2(l[0])
    wide = att.astype(F32)
    delta_out[0] = jnp.sum(wide * dot[0].astype(F32), axis=0, keepdims=True)
    for h in range(group):
        att_out[:, h * HD : (h + 1) * HD] = wide[:, h * tok : (h + 1) * tok].T.astype(BF16)


def backward_kernel(offs, first, last, tok, group, *refs):
    count = len(offs)
    info, qt, qn, dot, don, lse, delta, start = refs[:8]
    pairs = refs[8 : 8 + count]
    rest = refs[8 + count :]
    if not first:
        dq_in = rest[0]
        rest = rest[1:]
    outs = rest[:count]
    rest = rest[count:]
    if last:
        dq_out, dq = rest
    else:
        (dq,) = rest
    index, back = info[1], info[2]
    if first:
        dq[0] = jnp.zeros(dq.shape[1:], F32)
    else:
        dq[0] = dq_in[0]

    for off, pair, out in zip(offs, pairs, outs):

        @pl.when(off <= back)
        def _(off=off, pair=pair, out=out):
            key, value = pair[0, 0], pair[1, 0]
            scores = mm(key, qt[0])
            keep = allowed_of(start[...], off, index, tok, scores.shape)
            prob = jnp.exp2(jnp.where(keep, scores * C2 - lse[0], NEGATIVE))
            out[1, 0] = mm(prob.astype(BF16), don[0])
            dscore = (prob * (mm(value, dot[0]) - delta[0])).astype(BF16)
            out[0, 0] = mm(dscore, qn[0])
            dq[0] += mm_tn(key, dscore)

        @pl.when(off > back)
        def _(out=out):
            out[...] = jnp.zeros(out.shape, F32)

    if last:
        total = dq[0] * SCALE
        for h in range(group):
            dq_out[:, h * HD : (h + 1) * HD] = total[:, h * tok : (h + 1) * tok].T.astype(BF16)


def by_head(*shape):
    zeros = (0,) * (len(shape) - 1)
    return pl.BlockSpec((1, *shape[1:]), lambda g, info: (g, *zeros))


def forward(offs, first, tok, info, qt, pairs, state):
    kv_heads, _, wide = qt.shape
    row = by_head(kv_heads, 1, wide)
    square = by_head(kv_heads, HD, wide)
    own = pl.BlockSpec((2, 1, tok, HD), lambda g, info: (0, g, 0, 0))
    row_shape = jax.ShapeDtypeStruct((kv_heads, 1, wide), F32)
    return pl.pallas_call(
        functools.partial(forward_kernel, offs, first, tok),
        out_shape=[row_shape, row_shape, jax.ShapeDtypeStruct((kv_heads, HD, wide), F32)],
        grid_spec=pltpu.PrefetchScalarGridSpec(
            num_scalar_prefetch=1,
            grid=(kv_heads,),
            in_specs=[square] + [own] * len(offs) + ([] if first else [row, row, square]),
            out_specs=[row, row, square],
        ),
        compiler_params=pltpu.CompilerParams(dimension_semantics=("arbitrary",)),
        cost_estimate=pl.CostEstimate(
            flops=4 * len(offs) * kv_heads * tok * wide * HD,
            transcendentals=len(offs) * kv_heads * tok * wide,
            bytes_accessed=8 * kv_heads * HD * wide,
        ),
        name="forward",
    )(info, qt, *pairs, *([] if first else state))


def finish(offs, tok, info, qt, start, stack, pairs, state, dot):
    kv_heads, _, wide = qt.shape
    group = wide // tok
    row = by_head(kv_heads, 1, wide)
    square = by_head(kv_heads, HD, wide)
    own = pl.BlockSpec((2, 1, tok, HD), lambda g, info: (0, g, 0, 0))
    whole = pl.BlockSpec((stack.shape[0], 2, 1, tok, HD), lambda g, info: (0, 0, g, 0, 0))
    row_shape = jax.ShapeDtypeStruct((kv_heads, 1, wide), F32)
    return pl.pallas_call(
        functools.partial(finish_kernel, offs, tok, group),
        out_shape=[jax.ShapeDtypeStruct((tok, kv_heads * group * HD), BF16), row_shape, row_shape],
        grid_spec=pltpu.PrefetchScalarGridSpec(
            num_scalar_prefetch=1,
            grid=(kv_heads,),
            in_specs=[square, pl.BlockSpec((1, wide), lambda g, info: (0, 0)), whole]
            + [own] * len(offs)
            + [row, row, square, square],
            out_specs=[pl.BlockSpec((tok, group * HD), lambda g, info: (0, g)), row, row],
            scratch_shapes=[
                pltpu.VMEM((1, 1, wide), F32),
                pltpu.VMEM((1, 1, wide), F32),
                pltpu.VMEM((1, HD, wide), F32),
            ],
        ),
        compiler_params=pltpu.CompilerParams(dimension_semantics=("arbitrary",)),
        cost_estimate=pl.CostEstimate(
            flops=8 * kv_heads * tok * wide * HD,
            transcendentals=2 * kv_heads * tok * wide,
            bytes_accessed=8 * kv_heads * HD * wide,
        ),
        name="finish",
    )(info, qt, start, stack, *pairs, *state, dot)


def backward(offs, first, last, tok, info, qt, qn, dot, don, lse, delta, start, pairs, dq):
    kv_heads, _, wide = qt.shape
    group = wide // tok
    row = by_head(kv_heads, 1, wide)
    square = by_head(kv_heads, HD, wide)
    tall = by_head(kv_heads, wide, HD)
    own = pl.BlockSpec((2, 1, tok, HD), lambda g, info: (0, g, 0, 0))
    in_specs = [square, tall, square, tall, row, row, pl.BlockSpec((1, wide), lambda g, info: (0, 0))]
    in_specs += [own] * len(offs)
    args = [qt, qn, dot, don, lse, delta, start, *pairs]
    if not first:
        in_specs.append(square)
        args.append(dq)
    out_specs = [own] * len(offs)
    out_shape = [jax.ShapeDtypeStruct((2, kv_heads, tok, HD), F32)] * len(offs)
    scratch = []
    if last:
        out_specs.append(pl.BlockSpec((tok, group * HD), lambda g, info: (0, g)))
        out_shape.append(jax.ShapeDtypeStruct((tok, kv_heads * group * HD), BF16))
        scratch = [pltpu.VMEM((1, HD, wide), F32)]
    else:
        out_specs.append(square)
        out_shape.append(jax.ShapeDtypeStruct((kv_heads, HD, wide), F32))
    return pl.pallas_call(
        functools.partial(backward_kernel, offs, first, last, tok, group),
        out_shape=out_shape,
        grid_spec=pltpu.PrefetchScalarGridSpec(
            num_scalar_prefetch=1,
            grid=(kv_heads,),
            in_specs=in_specs,
            out_specs=out_specs,
            scratch_shapes=scratch,
        ),
        compiler_params=pltpu.CompilerParams(dimension_semantics=("arbitrary",)),
        cost_estimate=pl.CostEstimate(
            flops=10 * len(offs) * kv_heads * tok * wide * HD,
            transcendentals=len(offs) * kv_heads * tok * wide,
            bytes_accessed=12 * kv_heads * HD * wide,
        ),
        name="backward",
    )(info, *args)


def backward_calls(reach):
    kept = [tuple(o for o in offs if o <= reach) for offs in BACKWARD_CALLS]
    kept = [offs for offs in kept if offs]
    return [(o,) for o in range(reach, kept[0][0], -1)] + kept


def length_route(devices, first):
    if first:
        return [(2 * ((i + 1) % devices) + 1, 2 * i + 1) for i in range(devices)]
    return [(2 * ((i + 2) % devices) + c, 2 * i + c) for i in range(devices) for c in range(2)]


def start_of_documents(heard, tok, devices, index):
    half = len(heard)
    mine = jnp.concatenate(heard)
    theirs = lax.ppermute(mine, "head", [(0, 1), (1, 0)])
    core = lax.axis_index("head")
    steps = 2 * jnp.arange(half, dtype=jnp.int32)
    owners = jnp.concatenate([index + core + steps, index + 1 - core + steps]) % devices
    every = jnp.concatenate([mine, theirs]).reshape(-1)
    each = mine.shape[1]
    numbers = (owners[:, None] * each + jnp.arange(each, dtype=jnp.int32)[None]).reshape(-1)
    ends = jnp.sum(jnp.where(numbers[None] <= numbers[:, None], every[None], 0), axis=1)
    position = index * tok + jnp.arange(tok, dtype=jnp.int32)
    return jnp.max(jnp.where(ends[None] <= position[:, None], ends[None], 0), axis=1)


def shards(query_rows, key_rows, value_rows, grad_out, lengths):
    tok = query_rows.shape[0]
    kv_heads = key_rows.shape[1] // HD
    q_heads = query_rows.shape[1] // HD
    group = q_heads // kv_heads
    wide = group * tok
    devices = lax.axis_size("seq")
    index = lax.axis_index("seq")
    assert MOST % tok == 0
    edge = MOST // tok
    beyond = devices - edge
    reach = max(edge, beyond) - 1
    up = [(i, (i + 1) % devices) for i in range(devices)]
    down = [((i + 1) % devices, i) for i in range(devices)]

    def heads_apart(rows):
        return rows.reshape(tok, kv_heads, HD).transpose(1, 0, 2)

    def heads_together(blocks):
        return blocks.transpose(1, 0, 2).reshape(tok, kv_heads * HD)

    pairs = [jnp.stack([heads_apart(key_rows), heads_apart(value_rows)])]
    half = devices // 2
    assert devices % 2 == 0 and lax.axis_size("head") == 2
    heard = []
    for step in range(max(reach, half)):
        if step == 0:
            next_lengths = lax.ppermute(lengths[None], ("seq", "head"), length_route(devices, True))
            heard.append(jnp.where(lax.axis_index("head") == 0, lengths[None], next_lengths))
        elif step < half:
            heard.append(lax.ppermute(heard[-1], ("seq", "head"), length_route(devices, False)))
        if step < reach:
            pairs.append(lax.ppermute(pairs[-1], "seq", up))
            heard[-1], pairs[-1] = lax.optimization_barrier((heard[-1], pairs[-1]))

    four = query_rows.reshape(tok, kv_heads, group, HD)
    grad_four = grad_out.reshape(tok, kv_heads, group, HD)
    qt = four.transpose(1, 3, 2, 0).reshape(kv_heads, HD, wide)
    qn = four.transpose(1, 2, 0, 3).reshape(kv_heads, wide, HD)
    dot = grad_four.transpose(1, 3, 2, 0).reshape(kv_heads, HD, wide)
    don = grad_four.transpose(1, 2, 0, 3).reshape(kv_heads, wide, HD)

    within = jnp.where(index < edge, index, -1)
    early = jnp.stack([within, index]).astype(jnp.int32)
    state = None
    for at in range(0, reach, FORWARD_SIZE):
        offs = tuple(range(at, min(at + FORWARD_SIZE, reach)))
        state = forward(offs, at == 0, tok, early, qt, [pairs[o] for o in offs], state)

    starts = start_of_documents(heard, tok, devices, index)
    back = index - starts[0] // tok
    info = jnp.stack([within, index, back]).astype(jnp.int32)
    start = jnp.tile(starts[None], (1, group))
    attended, lse, delta = finish(
        (reach,), tok, info, qt, start, jnp.stack(pairs[:beyond]), [pairs[reach]], state, dot
    )

    groups = backward_calls(reach)
    fresh = {}
    dq = None
    moving = None

    def run(n, dq):
        offs = groups[n]
        *grads, dq = backward(
            offs, n == 0, n == len(groups) - 1, tok, info, qt, qn, dot, don, lse, delta, start,
            [pairs[o] for o in offs], dq,
        )
        fresh.update(zip(offs, grads))
        return dq

    dq = run(0, dq)
    if len(groups) > 1:
        dq = run(1, dq)
    for n, offs in enumerate(groups):
        for off in offs:
            if moving is not None and off == offs[0] and 0 < n < len(groups) - 1:
                dq, moving = lax.optimization_barrier((dq, moving))
                dq = run(n + 1, dq)
            total = fresh[off]
            if moving is not None:
                total = total + moving.astype(F32)
            if off:
                moving = lax.ppermute(total.astype(BF16), "seq", down)
    key_out = heads_together((total[0] * SCALE).astype(BF16))
    value_out = heads_together(total[1].astype(BF16))
    return attended, dq, key_out, value_out


def solution(mesh):
    rows = P(("groups", "seq"), "head")
    return jax.shard_map(
        shards,
        mesh=mesh,
        in_specs=(rows, rows, rows, rows, P(("groups", "seq"))),
        out_specs=(rows, rows, rows, rows),
        check_vma=False,
    )
```

```python
import functools
import math

import jax
import jax.numpy as jnp
from jax import lax
from jax.experimental import pallas as pl
from jax.experimental.pallas import tpu as pltpu
from jax.sharding import PartitionSpec as P

HD = 128
MOST = 2176
NEGATIVE = -1e30
SCALE = 1.0 / math.sqrt(HD)
LOG2E = math.log2(math.e)
C2 = SCALE * LOG2E

F32 = jnp.float32
BF16 = jnp.bfloat16

FORWARD_SIZE = 4
BACKWARD_CALLS = ((16,), (15, 14), (13, 12, 11), (10, 9, 8), (7, 6, 5), (4, 3, 2), (1, 0))


def mm(a, b):
    return jnp.dot(a, b, preferred_element_type=F32)


def mm_tn(a, b):
    return lax.dot_general(a, b, (((0,), (0,)), ((), ())), preferred_element_type=F32)


def allowed_of(start, off, index, tok, shape):
    key = lax.broadcasted_iota(jnp.int32, shape, 0)
    keep = key >= start - (index - off) * tok
    if off == 0:
        query = lax.broadcasted_iota(jnp.int32, shape, 1) % tok
        keep = keep & (key <= query)
    return keep


def visit(key, value, qt, keep, m, l, acc):
    scores = mm(key, qt[0])
    if keep is not None:
        scores = jnp.where(keep, scores, NEGATIVE)
    old = m[0]
    new = jnp.maximum(old, jnp.max(scores, axis=0, keepdims=True))
    factor = jnp.exp2((old - new) * C2)
    expo = jnp.exp2((scores - new) * C2)
    m[0] = new
    l[0] = l[0] * factor + jnp.sum(expo, axis=0, keepdims=True)
    acc[0] = acc[0] * factor + mm_tn(value, expo.astype(BF16))


def clear(m, l, acc):
    m[0] = jnp.full(m.shape[1:], NEGATIVE, F32)
    l[0] = jnp.zeros(l.shape[1:], F32)
    acc[0] = jnp.zeros(acc.shape[1:], F32)


def forward_kernel(offs, first, tok, *refs):
    count = len(offs)
    info, qt = refs[:2]
    pairs = refs[2 : 2 + count]
    rest = refs[2 + count :]
    m, l, acc = rest[-3:]
    if first:
        clear(m, l, acc)
    else:
        for here, there in zip(rest[-3:], rest[:3]):
            here[0] = there[0]

    for off, pair in zip(offs, pairs):

        @pl.when(off <= info[0])
        def _(off=off, pair=pair):
            keep = None
            if off == 0:
                shape = (tok, qt.shape[-1])
                keep = lax.broadcasted_iota(jnp.int32, shape, 0) <= lax.broadcasted_iota(jnp.int32, shape, 1) % tok
            visit(pair[0, 0], pair[1, 0], qt, keep, m, l, acc)


def finish_kernel(offs, tok, group, *refs):
    count = len(offs)
    info, qt, start, stack = refs[:4]
    pairs = refs[4 : 4 + count]
    m_in, l_in, acc_in, dot, att_out, lse_out, delta_out, m, l, acc = refs[4 + count :]
    within, index, back = info[0], info[1], info[2]

    @pl.when(within >= 0)
    def _():
        m[0] = m_in[0]
        l[0] = l_in[0]
        acc[0] = acc_in[0]
        for off, pair in zip(offs, pairs):

            @pl.when(off <= within)
            def _(pair=pair):
                visit(pair[0, 0], pair[1, 0], qt, None, m, l, acc)

    @pl.when(within < 0)
    def _():
        clear(m, l, acc)

        def turn(off, _):
            shape = (tok, qt.shape[-1])
            key = lax.broadcasted_iota(jnp.int32, shape, 0)
            query = lax.broadcasted_iota(jnp.int32, shape, 1) % tok
            keep = (key >= start[...] - (index - off) * tok) & (key <= query + off * tok)
            visit(stack[off, 0, 0], stack[off, 1, 0], qt, keep, m, l, acc)
            return 0

        lax.fori_loop(0, jnp.minimum(back, stack.shape[0] - 1) + 1, turn, 0)

    att = (acc[0] / l[0]).astype(BF16)
    lse_out[0] = m[0] * C2 + jnp.log2(l[0])
    wide = att.astype(F32)
    delta_out[0] = jnp.sum(wide * dot[0].astype(F32), axis=0, keepdims=True)
    for h in range(group):
        att_out[:, h * HD : (h + 1) * HD] = wide[:, h * tok : (h + 1) * tok].T.astype(BF16)


def backward_kernel(offs, first, last, tok, group, *refs):
    count = len(offs)
    info, qt, qn, dot, don, lse, delta, start = refs[:8]
    pairs = refs[8 : 8 + count]
    rest = refs[8 + count :]
    if not first:
        dq_in = rest[0]
        rest = rest[1:]
    outs = rest[:count]
    rest = rest[count:]
    if last:
        dq_out, dq = rest
    else:
        (dq,) = rest
    index, back = info[1], info[2]
    if first:
        dq[0] = jnp.zeros(dq.shape[1:], F32)
    else:
        dq[0] = dq_in[0]

    for off, pair, out in zip(offs, pairs, outs):

        @pl.when(off <= back)
        def _(off=off, pair=pair, out=out):
            key, value = pair[0, 0], pair[1, 0]
            scores = mm(key, qt[0])
            keep = allowed_of(start[...], off, index, tok, scores.shape)
            prob = jnp.exp2(jnp.where(keep, scores * C2 - lse[0], NEGATIVE))
            out[1, 0] = mm(prob.astype(BF16), don[0])
            dscore = (prob * (mm(value, dot[0]) - delta[0])).astype(BF16)
            out[0, 0] = mm(dscore, qn[0])
            dq[0] += mm_tn(key, dscore)

        @pl.when(off > back)
        def _(out=out):
            out[...] = jnp.zeros(out.shape, F32)

    if last:
        total = dq[0] * SCALE
        for h in range(group):
            dq_out[:, h * HD : (h + 1) * HD] = total[:, h * tok : (h + 1) * tok].T.astype(BF16)


def by_head(*shape):
    zeros = (0,) * (len(shape) - 1)
    return pl.BlockSpec((1, *shape[1:]), lambda g, info: (g, *zeros))


def forward(offs, first, tok, info, qt, pairs, state):
    kv_heads, _, wide = qt.shape
    row = by_head(kv_heads, 1, wide)
    square = by_head(kv_heads, HD, wide)
    own = pl.BlockSpec((2, 1, tok, HD), lambda g, info: (0, g, 0, 0))
    row_shape = jax.ShapeDtypeStruct((kv_heads, 1, wide), F32)
    return pl.pallas_call(
        functools.partial(forward_kernel, offs, first, tok),
        out_shape=[row_shape, row_shape, jax.ShapeDtypeStruct((kv_heads, HD, wide), F32)],
        grid_spec=pltpu.PrefetchScalarGridSpec(
            num_scalar_prefetch=1,
            grid=(kv_heads,),
            in_specs=[square] + [own] * len(offs) + ([] if first else [row, row, square]),
            out_specs=[row, row, square],
        ),
        compiler_params=pltpu.CompilerParams(dimension_semantics=("arbitrary",)),
        cost_estimate=pl.CostEstimate(
            flops=4 * len(offs) * kv_heads * tok * wide * HD,
            transcendentals=len(offs) * kv_heads * tok * wide,
            bytes_accessed=8 * kv_heads * HD * wide,
        ),
        name="forward",
    )(info, qt, *pairs, *([] if first else state))


def finish(offs, tok, info, qt, start, stack, pairs, state, dot):
    kv_heads, _, wide = qt.shape
    group = wide // tok
    row = by_head(kv_heads, 1, wide)
    square = by_head(kv_heads, HD, wide)
    own = pl.BlockSpec((2, 1, tok, HD), lambda g, info: (0, g, 0, 0))
    whole = pl.BlockSpec((stack.shape[0], 2, 1, tok, HD), lambda g, info: (0, 0, g, 0, 0))
    row_shape = jax.ShapeDtypeStruct((kv_heads, 1, wide), F32)
    return pl.pallas_call(
        functools.partial(finish_kernel, offs, tok, group),
        out_shape=[jax.ShapeDtypeStruct((tok, kv_heads * group * HD), BF16), row_shape, row_shape],
        grid_spec=pltpu.PrefetchScalarGridSpec(
            num_scalar_prefetch=1,
            grid=(kv_heads,),
            in_specs=[square, pl.BlockSpec((1, wide), lambda g, info: (0, 0)), whole]
            + [own] * len(offs)
            + [row, row, square, square],
            out_specs=[pl.BlockSpec((tok, group * HD), lambda g, info: (0, g)), row, row],
            scratch_shapes=[
                pltpu.VMEM((1, 1, wide), F32),
                pltpu.VMEM((1, 1, wide), F32),
                pltpu.VMEM((1, HD, wide), F32),
            ],
        ),
        compiler_params=pltpu.CompilerParams(dimension_semantics=("arbitrary",)),
        cost_estimate=pl.CostEstimate(
            flops=8 * kv_heads * tok * wide * HD,
            transcendentals=2 * kv_heads * tok * wide,
            bytes_accessed=8 * kv_heads * HD * wide,
        ),
        name="finish",
    )(info, qt, start, stack, *pairs, *state, dot)


def backward(offs, first, last, tok, info, qt, qn, dot, don, lse, delta, start, pairs, dq):
    kv_heads, _, wide = qt.shape
    group = wide // tok
    row = by_head(kv_heads, 1, wide)
    square = by_head(kv_heads, HD, wide)
    tall = by_head(kv_heads, wide, HD)
    own = pl.BlockSpec((2, 1, tok, HD), lambda g, info: (0, g, 0, 0))
    in_specs = [square, tall, square, tall, row, row, pl.BlockSpec((1, wide), lambda g, info: (0, 0))]
    in_specs += [own] * len(offs)
    args = [qt, qn, dot, don, lse, delta, start, *pairs]
    if not first:
        in_specs.append(square)
        args.append(dq)
    out_specs = [own] * len(offs)
    out_shape = [jax.ShapeDtypeStruct((2, kv_heads, tok, HD), F32)] * len(offs)
    scratch = []
    if last:
        out_specs.append(pl.BlockSpec((tok, group * HD), lambda g, info: (0, g)))
        out_shape.append(jax.ShapeDtypeStruct((tok, kv_heads * group * HD), BF16))
        scratch = [pltpu.VMEM((1, HD, wide), F32)]
    else:
        out_specs.append(square)
        out_shape.append(jax.ShapeDtypeStruct((kv_heads, HD, wide), F32))
    return pl.pallas_call(
        functools.partial(backward_kernel, offs, first, last, tok, group),
        out_shape=out_shape,
        grid_spec=pltpu.PrefetchScalarGridSpec(
            num_scalar_prefetch=1,
            grid=(kv_heads,),
            in_specs=in_specs,
            out_specs=out_specs,
            scratch_shapes=scratch,
        ),
        compiler_params=pltpu.CompilerParams(dimension_semantics=("arbitrary",)),
        cost_estimate=pl.CostEstimate(
            flops=10 * len(offs) * kv_heads * tok * wide * HD,
            transcendentals=len(offs) * kv_heads * tok * wide,
            bytes_accessed=12 * kv_heads * HD * wide,
        ),
        name="backward",
    )(info, *args)


def backward_calls(reach):
    kept = [tuple(o for o in offs if o <= reach) for offs in BACKWARD_CALLS]
    kept = [offs for offs in kept if offs]
    return [(o,) for o in range(reach, kept[0][0], -1)] + kept


def length_route(devices):
    turn = lambda i, c: (i + 1 - 2 * c) % devices
    return [(2 * i + c, 2 * turn(i, c) + c) for i in range(devices) for c in range(2)]


def start_of_documents(lengths, heard, tok, devices, index):
    half = len(heard)
    mine = jnp.concatenate(heard)
    theirs = lax.ppermute(mine, "head", [(0, 1), (1, 0)])
    sign = jnp.where(lax.axis_index("head") == 0, -1, 1)
    steps = jnp.arange(1, half + 1, dtype=jnp.int32)
    left = devices - 1 - half
    owners = jnp.concatenate([index[None], index + sign * steps, index - sign * steps[:left]]) % devices
    every = jnp.concatenate([lengths[None], mine, theirs[:left]]).reshape(-1)
    each = lengths.shape[0]
    numbers = (owners[:, None] * each + jnp.arange(each, dtype=jnp.int32)[None]).reshape(-1)
    ends = jnp.sum(jnp.where(numbers[None] <= numbers[:, None], every[None], 0), axis=1)
    position = index * tok + jnp.arange(tok, dtype=jnp.int32)
    return jnp.max(jnp.where(ends[None] <= position[:, None], ends[None], 0), axis=1)


def shards(query_rows, key_rows, value_rows, grad_out, lengths):
    tok = query_rows.shape[0]
    kv_heads = key_rows.shape[1] // HD
    q_heads = query_rows.shape[1] // HD
    group = q_heads // kv_heads
    wide = group * tok
    devices = lax.axis_size("seq")
    index = lax.axis_index("seq")
    assert MOST % tok == 0
    edge = MOST // tok
    beyond = devices - edge
    reach = max(edge, beyond) - 1
    up = [(i, (i + 1) % devices) for i in range(devices)]
    down = [((i + 1) % devices, i) for i in range(devices)]

    def heads_apart(rows):
        return rows.reshape(tok, kv_heads, HD).transpose(1, 0, 2)

    def heads_together(blocks):
        return blocks.transpose(1, 0, 2).reshape(tok, kv_heads * HD)

    pairs = [jnp.stack([heads_apart(key_rows), heads_apart(value_rows)])]
    half = devices // 2
    assert lax.axis_size("head") == 2
    assert reach == half
    heard = [lengths[None]]
    pairs = [pairs[0]]
    ring, passing = pairs[0], heard[0]
    for step in range(reach):
        heard.append(lax.ppermute(passing, ("seq", "head"), length_route(devices)))
        here = lax.ppermute(ring, "seq", up)
        ring, heard[-2] = lax.optimization_barrier((here, heard[-2]))
        passing, here = lax.optimization_barrier((heard[-1], here))
        pairs.append(here)

    four = query_rows.reshape(tok, kv_heads, group, HD)
    grad_four = grad_out.reshape(tok, kv_heads, group, HD)
    qt = four.transpose(1, 3, 2, 0).reshape(kv_heads, HD, wide)
    qn = four.transpose(1, 2, 0, 3).reshape(kv_heads, wide, HD)
    dot = grad_four.transpose(1, 3, 2, 0).reshape(kv_heads, HD, wide)
    don = grad_four.transpose(1, 2, 0, 3).reshape(kv_heads, wide, HD)

    within = jnp.where(index < edge, index, -1)
    early = jnp.stack([within, index]).astype(jnp.int32)
    state = None
    for at in range(0, reach, FORWARD_SIZE):
        offs = tuple(range(at, min(at + FORWARD_SIZE, reach)))
        state = forward(offs, at == 0, tok, early, qt, [pairs[o] for o in offs], state)

    starts = start_of_documents(lengths, heard[1:], tok, devices, index)
    back = index - starts[0] // tok
    info = jnp.stack([within, index, back]).astype(jnp.int32)
    start = jnp.tile(starts[None], (1, group))
    attended, lse, delta = finish(
        (reach,), tok, info, qt, start, jnp.stack(pairs[:beyond]), [pairs[reach]], state, dot
    )

    groups = backward_calls(reach)
    fresh = {}
    dq = None
    moving = None

    def run(n, dq):
        offs = groups[n]
        *grads, dq = backward(
            offs, n == 0, n == len(groups) - 1, tok, info, qt, qn, dot, don, lse, delta, start,
            [pairs[o] for o in offs], dq,
        )
        fresh.update(zip(offs, grads))
        return dq

    dq = run(0, dq)
    if len(groups) > 1:
        dq = run(1, dq)
    for n, offs in enumerate(groups):
        for off in offs:
            if moving is not None and off == offs[0] and 0 < n < len(groups) - 1:
                dq, moving = lax.optimization_barrier((dq, moving))
                dq = run(n + 1, dq)
            total = fresh[off]
            if moving is not None:
                total = total + moving.astype(F32)
            if off:
                moving = lax.ppermute(total.astype(BF16), "seq", down)
    key_out = heads_together((total[0] * SCALE).astype(BF16))
    value_out = heads_together(total[1].astype(BF16))
    return attended, dq, key_out, value_out


def solution(mesh):
    rows = P(("groups", "seq"), "head")
    return jax.shard_map(
        shards,
        mesh=mesh,
        in_specs=(rows, rows, rows, rows, P(("groups", "seq"))),
        out_specs=(rows, rows, rows, rows),
        check_vma=False,
    )
```
